32 devices in a mesh: expert: 2 (over x), dp: 16 (over z, y, core).
Axes of the slice: x: 2, y: 2, z: 4, core: 2. Of those that a mesh axis runs over, the one named last changes fastest.
Arguments:
- upstream: bfloat16 [4096, 3584], P(('expert', 'dp')), may hold values from -2.5 to 2.5
- combine_weights: bfloat16 [4096, 2], P(('expert', 'dp')), may hold values from 0.099609375 to 1
- expert_ids: int32 [4096, 2], P(('expert', 'dp')), may hold values from 0 to 1, as said below
- saved_hidden: bfloat16 [2, 4096, 2048], P('expert', 'dp'), may hold values from -6 to 6
- down_weight: bfloat16 [2, 1024, 3584], P('expert'), may hold values from -0.1875 to 0.1875
Outputs:
- grad_down: float32 [2, 3584, 1024], P('expert', 'dp')
- grad_hidden: bfloat16 [2, 4096, 2048], P('expert', 'dp')
- grad_probs: float32 [4096, 2], P(('expert', 'dp'))
The draws below stay inside these ranges and needn't reach their ends.
Inputs may be any that keep to these rules, and one draw needn't show every extreme that they name: `expert_ids`: the 2 ids of a token differ. Among the 128 tokens of one device no expert is named more than 128 times, and in every draw one expert is named exactly 128 times by the tokens of every device.
All inputs are finite; a program needn't handle non-finite values.
Results may differ from the reference program's by a relative error of at most 0.0049.
Values may be sent and summed in bfloat16 or wider, within the bound.
No kernel may reach another device: no remote copies, remote signals or barrier semaphores. Data moves between devices by JAX's collectives and lax.ppermute only.
A program may use at most 128 MiB of HBM per device.

```python
import jax
import jax.numpy as jnp
from jax import lax

D = 3584
FF = 1024
TOPK = 2
TOK_DEV = 128
EXPERTS = 2
CAP = 128
ROWS_E = 256
TOKENS = 4096
N_DP = 16


def draw_expert_ids(key, part):
    blocks = TOKENS // TOK_DEV
    others = max(EXPERTS - 1, 1)
    subkeys = jax.random.split(key, 5)
    favored = jax.random.randint(subkeys[0], (), 0, EXPERTS)
    ranking = jax.vmap(lambda block_key: jax.random.permutation(block_key, TOK_DEV))(jax.random.split(subkeys[1], blocks))
    first_offset = jax.random.randint(subkeys[2], (blocks, 1), 0, others)
    stride = jax.random.randint(subkeys[3], (blocks, 1), 1, max(others, 2))
    first_other = (first_offset + ranking - CAP) % others
    second_other = (first_offset - CAP + stride + ranking) % others
    first_choice = jnp.where(ranking < CAP, favored, (favored + 1 + first_other) % EXPERTS)
    second_choice = (favored + 1 + second_other) % EXPERTS
    flipped = jax.random.randint(subkeys[4], (blocks, TOK_DEV), 0, 2) == 1
    column_a = jnp.where(flipped, second_choice, first_choice)
    column_b = jnp.where(flipped, first_choice, second_choice)
    return jnp.stack([column_a, column_b], axis=-1).reshape(TOKENS, TOPK).astype(jnp.int32)


def strengthened(array, rng, source, target, parts, factor):
    owner, partner = [(jnp.arange(array.shape[dim]) // (array.shape[dim] // parts)).reshape([-1 if axis == dim else 1 for axis in range(array.ndim)]) for dim in (source, target)]
    chosen = jax.random.permutation(rng, parts)[partner]
    strong = (owner == chosen) | (owner == (partner + parts // 2) % parts)
    return jnp.where(strong, factor * array, array)


def steps_of(own_key, shape, shards, smallest, top_value):
    loudness, own = 1.0, jax.random.fold_in(own_key, 6)
    for position, shards_of in shards:
        draws = jnp.exp(jax.random.uniform(jax.random.fold_in(own, position), (shards_of,), jnp.float32, smallest / len(shards), top_value / len(shards)))
        loudness = loudness * jnp.repeat(draws, shape[position] // shards_of).reshape([-1 if axis == position else 1 for axis in range(len(shape))])
    return loudness


def centred(stream_key, extent, width, most, shards=(), kind=jnp.bfloat16):
    array = width * jax.random.normal(stream_key, extent, jnp.float32)
    if shards:
        array = array * steps_of(stream_key, extent, shards, -0.22, 0.18)
    return jnp.clip(array, -most, most).astype(kind)


def heavy_noise(own_key, shape, scale, reach, shards, heavy, held_as=jnp.bfloat16):
    values = scale * jax.random.normal(own_key, shape, jnp.float32)
    if shards:
        values = values * steps_of(own_key, shape, shards, -0.22, 0.18)
    return jnp.clip(strengthened(values, jax.random.fold_in(own_key, 3), *heavy), -reach, reach).astype(held_as)


def setup_inputs(seed: int = 0) -> dict:
    key_of = jax.random.split(jax.random.key(seed), 6)
    upstream = heavy_noise(key_of[0], (TOKENS, D), 0.25, 2.5, ((0, 32),), (0, 1, 32, 2.75))
    combine_weights = jnp.clip(0.099609375 + 0.9003906 * jax.random.uniform(key_of[1], (TOKENS, TOPK), jnp.float32) ** steps_of(key_of[1], (TOKENS, TOPK), ((0, 32),), -0.2, 0.2), 0.099609375, 1.0).astype(jnp.bfloat16)
    expert_ids = draw_expert_ids(jax.random.fold_in(key_of[5], 71), 0)
    saved_hidden = centred(key_of[3], (EXPERTS, N_DP * ROWS_E, 2 * FF), 1.0, 6.0, ((0, 2), (1, 16)))
    down_weight = centred(key_of[4], (EXPERTS, FF, D), FF ** -0.5, 0.1875, ((0, 2),))
    return dict(upstream=upstream, combine_weights=combine_weights, expert_ids=expert_ids, saved_hidden=saved_hidden, down_weight=down_weight)


def reference(upstream, combine_weights, expert_ids, saved_hidden, down_weight):
    blocks = TOKENS // TOK_DEV
    block_ids = expert_ids.reshape(blocks, TOK_DEV, TOPK)
    block_weights = combine_weights.astype(jnp.float32).reshape(blocks, TOK_DEV, TOPK)
    block_index = jnp.arange(blocks, dtype=jnp.int32)
    base_row = (block_index % N_DP) * ROWS_E + (block_index // N_DP) * CAP
    total_rows = N_DP * ROWS_E

    def one_expert(expert_index):
        matched = block_ids == expert_index
        member = jnp.any(matched, axis=2).astype(jnp.int32)
        slot_rank = jnp.cumsum(member, axis=1) - member
        target = jnp.where(member == 1, base_row[:, None] + slot_rank, total_rows).reshape(-1).astype(jnp.int32)
        weight_in = jnp.sum(jnp.where(matched, block_weights, 0.0), axis=2).reshape(-1)
        routed = jnp.zeros((total_rows, D), jnp.bfloat16).at[target].set(upstream, mode="drop")
        row_weight = jnp.zeros((total_rows,), jnp.float32).at[target].set(weight_in, mode="drop")
        stored = saved_hidden[expert_index].astype(jnp.float32)
        gate_pre = stored[:, :FF]
        up_pre = stored[:, FF:]
        sigmoid_gate = jax.nn.sigmoid(gate_pre)
        activated = (gate_pre * sigmoid_gate * up_pre).astype(jnp.bfloat16)
        scaled = (row_weight[:, None] * routed.astype(jnp.float32)).astype(jnp.bfloat16)
        weights = down_weight[expert_index]
        grad_weight = jnp.dot(scaled.T, activated, preferred_element_type=jnp.float32)
        backward = jnp.dot(routed, weights.T, preferred_element_type=jnp.float32)
        grad_act = row_weight[:, None] * backward
        grad_gate = grad_act * up_pre * sigmoid_gate * (1.0 + gate_pre * (1.0 - sigmoid_gate))
        grad_up = grad_act * gate_pre * sigmoid_gate
        grad_hidden = jnp.concatenate([grad_gate, grad_up], axis=1).astype(jnp.bfloat16)
        scores = jnp.sum(backward * activated.astype(jnp.float32), axis=1)
        picked = jnp.take(scores, jnp.minimum(target, total_rows - 1)).reshape(blocks, TOK_DEV)
        share = jnp.where(matched, picked[:, :, None], 0.0)
        return grad_weight, grad_hidden, share

    grad_down, grad_hidden, shares = lax.map(one_expert, jnp.arange(EXPERTS, dtype=jnp.int32))
    grad_probs = jnp.sum(shares, axis=0).reshape(TOKENS, TOPK)
    return grad_down, grad_hidden, grad_probs
```

```python
import functools

import jax
import jax.numpy as jnp
from jax import lax
from jax.experimental import pallas as pl
from jax.experimental.pallas import tpu as pltpu
from jax.sharding import PartitionSpec as P

INNER = 4
LANES = 128
VMEM = pl.BlockSpec(memory_space=pltpu.VMEM)


def contract_rows(left_rows, right_rows):
    return lax.dot_general(
        left_rows, right_rows, (((0,), (0,)), ((), ())), preferred_element_type=jnp.float32
    )


def call(kernel, outs, *args, scratch=()):
    return pl.pallas_call(
        kernel,
        out_shape=outs,
        in_specs=[VMEM] * len(args),
        out_specs=jax.tree.map(lambda _: VMEM, outs),
        scratch_shapes=list(scratch),
        compiler_params=pltpu.CompilerParams(vmem_limit_bytes=48 << 20),
    )(*args)


def token_weight(ids_ref, weights_ref, expert):
    picked = jnp.where(ids_ref[...] == expert, weights_ref[...].astype(jnp.float32), 0.0)
    return jnp.sum(picked, axis=1, keepdims=True)


def chunk_start(k, chunk):
    group = lax.axis_index("dp") // INNER
    return pl.multiple_of((group ^ k) * chunk, LANES)


def first_kernel(k, chunk, up_ref, ids_ref, weights_ref, out_ref):
    out_ref[:, :chunk] = up_ref[:, pl.ds(chunk_start(k, chunk), chunk)]
    weight = token_weight(ids_ref, weights_ref, 1 - lax.axis_index("expert"))
    out_ref[:, chunk:] = jnp.broadcast_to(weight, (weight.shape[0], LANES)).astype(jnp.bfloat16)


def own_kernel(outer, chunk, up_ref, ids_ref, weights_ref, *outs):
    own_refs, send_refs = outs[:outer], outs[outer:]
    weight = token_weight(ids_ref, weights_ref, lax.axis_index("expert"))
    for k in range(outer):
        rows = up_ref[:, pl.ds(chunk_start(k, chunk), chunk)]
        if k < outer - 1:
            send_refs[k][...] = rows
        scaled = (weight * rows.astype(jnp.float32)).astype(jnp.bfloat16)
        own_refs[k][...] = scaled.T


def act_kernel(hidden_ref, out_ref):
    rows, hidden_units = out_ref.shape
    half = rows // 2
    expert = lax.axis_index("expert")
    for part in range(2):
        source = pl.ds(pl.multiple_of((expert ^ part) * half, half), half)
        gate = hidden_ref[source, :hidden_units].astype(jnp.float32)
        up = hidden_ref[source, hidden_units:].astype(jnp.float32)
        act = gate * jax.nn.sigmoid(gate) * up
        out_ref[part * half : (part + 1) * half, :] = act.astype(jnp.bfloat16)


def split_kernel(chunk, got_ref, first_ref, own_ref, *refs):
    pays, scaled_ref = refs[:INNER], refs[INNER]
    weight = first_ref[:, chunk : chunk + 1].astype(jnp.float32)
    scaled = (weight * got_ref[:, :chunk].astype(jnp.float32)).astype(jnp.bfloat16)
    scaled_ref[...] = scaled.T
    piece = chunk // INNER
    mine = lax.axis_index("dp") % INNER
    for j in range(INNER):
        rows = pl.ds(pl.multiple_of((mine ^ j) * piece, 16), piece)
        pays[j][:, :LANES] = own_ref[rows, :]
        pays[j][:, LANES:] = scaled_ref[rows, :]


def partial_kernel(*refs):
    pays, acts, adds, out_ref = refs[:INNER], refs[INNER : 2 * INNER], refs[2 * INNER : -1], refs[-1]
    total = None
    for pay, act in zip(pays, acts):
        term = jnp.dot(pay[...], act[...], preferred_element_type=jnp.float32)
        total = term if total is None else total + term
    for add in adds:
        total = total + add[...].astype(jnp.float32)
    out_ref[...] = total.astype(out_ref.dtype)


def hidden_kernel(outer, chunk, up_ref, ids_ref, weights_ref, hidden_ref, w_ref, *refs):
    got_refs, out_ref, own_score, got_score = refs[:outer], refs[outer], refs[outer + 1], refs[outer + 2]
    step = pl.program_id(0)
    half = up_ref.shape[0]
    width = w_ref.shape[0]
    hidden_units = hidden_ref.shape[1] // 2
    expert = lax.axis_index("expert")
    last = got_refs[outer - 1]

    @pl.when(step == 0)
    def _():
        own_score[...] = jnp.zeros_like(own_score)
        got_score[...] = jnp.zeros_like(got_score)

    def finish(backward, weight, part, score):
        rows = pl.ds(pl.multiple_of((expert ^ part) * half, half), half)
        gate_cols = pl.ds(pl.multiple_of(step * width, LANES), width)
        up_cols = pl.ds(pl.multiple_of(hidden_units + step * width, LANES), width)
        gate = hidden_ref[rows, gate_cols].astype(jnp.float32)
        up = hidden_ref[rows, up_cols].astype(jnp.float32)
        sig = jax.nn.sigmoid(gate)
        act = (gate * sig * up).astype(jnp.bfloat16).astype(jnp.float32)
        score[...] += jnp.sum(backward * act, axis=1, keepdims=True)
        grad = weight * backward
        out_ref[rows, gate_cols] = (grad * up * sig * (1.0 + gate * (1.0 - sig))).astype(jnp.bfloat16)
        out_ref[rows, up_cols] = (grad * gate * sig).astype(jnp.bfloat16)

    turned = (((1,), (1,)), ((), ()))
    own = lax.dot_general(up_ref[...], w_ref[...], turned, preferred_element_type=jnp.float32)
    finish(own, token_weight(ids_ref, weights_ref, expert), 0, own_score)
    got = None
    for k in range(outer):
        cols = w_ref[:, pl.ds(chunk_start(k, chunk), chunk)]
        term = lax.dot_general(got_refs[k][:, :chunk], cols, turned, preferred_element_type=jnp.float32)
        got = term if got is None else got + term
    finish(got, last[:, chunk : chunk + 1].astype(jnp.float32), 1, got_score)


def hidden_call(outer, chunk, upstream, ids, combine, stored, weights, got):
    tokens, features = upstream.shape
    hidden_units = weights.shape[0]
    width = 256
    whole = lambda a: pl.BlockSpec(a.shape, lambda i: (0, 0))
    column = jax.ShapeDtypeStruct((tokens, 1), jnp.float32)
    return pl.pallas_call(
        functools.partial(hidden_kernel, outer, chunk),
        grid=(hidden_units // width,),
        out_shape=(jax.ShapeDtypeStruct(stored.shape, jnp.bfloat16), column, column),
        in_specs=[whole(upstream), whole(ids), whole(combine), whole(stored)]
        + [pl.BlockSpec((width, features), lambda i: (i, 0))]
        + [whole(g) for g in got],
        out_specs=(whole(stored), whole(column), whole(column)),
        compiler_params=pltpu.CompilerParams(vmem_limit_bytes=48 << 20),
    )(upstream, ids, combine, stored, weights, *got)


def both_experts(upstream, combine_weights, expert_ids, saved_hidden, down_weight):
    tokens, features = upstream.shape
    n = lax.axis_size("dp")
    outer = n // INNER
    chunk, piece = features // outer, features // n
    hidden_units = down_weight.shape[1]
    stored, weights = saved_hidden[0], down_weight[0]
    bf16 = lambda *shape: jax.ShapeDtypeStruct(shape, jnp.bfloat16)
    flip = [(0, 1), (1, 0)]
    swap = lambda bit: [(i, i ^ bit) for i in range(n)]

    top = outer - 1
    first = call(
        functools.partial(first_kernel, top, chunk),
        bf16(tokens, chunk + LANES), upstream, expert_ids, combine_weights,
    )
    got = {top: lax.ppermute(first, "expert", flip)}
    act = {0: call(act_kernel, bf16(stored.shape[0], hidden_units), stored)}
    act[2] = lax.ppermute(act[0], "dp", swap(2))
    own = call(
        functools.partial(own_kernel, outer, chunk),
        (bf16(chunk, tokens),) * outer + (bf16(tokens, chunk),) * top,
        upstream, expert_ids, combine_weights,
    )
    own, send = own[:outer], own[outer:]
    for k in range(top - 1, -1, -1):
        got[k] = lax.ppermute(send[k], "expert", flip)
    act[1] = lax.ppermute(act[0], "dp", swap(1))
    act[3] = lax.ppermute(act[2], "dp", swap(1))

    adds = {k: [] for k in range(outer)}
    for k in range(top, -1, -1):
        pays = call(
            functools.partial(split_kernel, chunk),
            (bf16(piece, 2 * tokens),) * INNER, got[k], got[top], own[k],
            scratch=[pltpu.VMEM((chunk, tokens), jnp.bfloat16)],
        )
        pays = [pays[0]] + [lax.ppermute(pays[j], "dp", swap(j)) for j in range(1, INNER)]
        kind = jnp.bfloat16 if k else jnp.float32
        terms = adds[k] if k else []
        part = call(
            partial_kernel, jax.ShapeDtypeStruct((piece, hidden_units), kind),
            *pays, *[act[j] for j in range(INNER)], *terms,
        )
        if k:
            bit = k & -k
            adds[k ^ bit].append(lax.ppermute(part, "dp", swap(bit * INNER)))
    grad_down = part
    for term in adds[0]:
        grad_down = grad_down + term.astype(jnp.float32)

    grad_hidden, own_score, got_score = hidden_call(
        outer, chunk, upstream, expert_ids, combine_weights, stored, weights,
        [got[k] for k in range(outer)],
    )
    back_score = lax.ppermute(got_score, "expert", flip)
    grad_probs = jnp.where(expert_ids == lax.axis_index("expert"), own_score, back_score)
    return grad_down[None], grad_hidden[None], grad_probs


def any_experts(upstream, combine_weights, expert_ids, saved_hidden, down_weight):
    tok_rows, features = upstream.shape
    experts = lax.axis_size("expert")
    hidden_units = down_weight.shape[1]
    capacity = saved_hidden.shape[1] // experts
    labels = lax.broadcasted_iota(jnp.int32, (1, 1, experts), 2)
    matched = expert_ids[:, :, None] == labels
    member = jnp.sum(matched.astype(jnp.int32), axis=1)
    slot_rank = jnp.cumsum(member, axis=0) - member
    token_iota = lax.broadcasted_iota(jnp.int32, (tok_rows, experts, capacity), 0)
    slot_iota = lax.broadcasted_iota(jnp.int32, (tok_rows, experts, capacity), 2)
    placed = (member[:, :, None] == 1) & (slot_rank[:, :, None] == slot_iota)
    source = jnp.sum(jnp.where(placed, token_iota, 0), axis=0)
    filled = jnp.any(placed, axis=0)
    token_weight = jnp.sum(
        jnp.where(matched, combine_weights[:, :, None].astype(jnp.float32), 0.0), axis=1
    )
    send_rows = jnp.where(filled[:, :, None], upstream[source], jnp.zeros((), jnp.bfloat16))
    send_weight = jnp.where(
        filled, jnp.take_along_axis(token_weight.T, source, axis=1), 0.0
    ).astype(jnp.bfloat16)
    got_rows, got_weight = (
        lax.all_to_all(send_rows, "expert", split_axis=0, concat_axis=0, tiled=True),
        lax.all_to_all(send_weight, "expert", split_axis=0, concat_axis=0, tiled=True),
    )
    routed = got_rows.reshape(experts * capacity, features)
    row_weight = got_weight.reshape(experts * capacity, 1).astype(jnp.float32)
    stored = saved_hidden[0]
    gate_pre = stored[:, :hidden_units].astype(jnp.float32)
    up_pre = stored[:, hidden_units:].astype(jnp.float32)
    sigmoid_gate = jax.nn.sigmoid(gate_pre)
    activated = (gate_pre * sigmoid_gate * up_pre).astype(jnp.bfloat16)
    scaled = (row_weight * routed.astype(jnp.float32)).astype(jnp.bfloat16)
    weights = down_weight[0]
    backward = lax.dot_general(
        routed, weights, (((1,), (1,)), ((), ())), preferred_element_type=jnp.float32
    )
    grad_act = row_weight * backward
    grad_gate = grad_act * up_pre * sigmoid_gate * (1.0 + gate_pre * (1.0 - sigmoid_gate))
    grad_up = grad_act * gate_pre * sigmoid_gate
    grad_hidden = jnp.concatenate([grad_gate, grad_up], axis=1).astype(jnp.bfloat16)
    outputs = jnp.dot(activated, weights, preferred_element_type=jnp.float32)
    scores = jnp.sum(routed.astype(jnp.float32) * outputs, axis=1)
    returned = lax.all_to_all(
        scores.reshape(experts, capacity), "expert", split_axis=0, concat_axis=0, tiled=True
    )
    slot_of = jnp.sum(jnp.where(matched, slot_rank[:, None, :], 0), axis=2)
    flat_index = expert_ids * capacity + slot_of
    score_table = returned.reshape(experts * capacity)
    cell_ids = lax.broadcasted_iota(jnp.int32, (1, 1, experts * capacity), 2)
    grad_probs = jnp.sum(
        jnp.where(flat_index[:, :, None] == cell_ids, score_table[None, None, :], 0.0), axis=2
    )
    grad_down = lax.psum_scatter(
        contract_rows(scaled, activated), "dp", scatter_dimension=0, tiled=True
    )
    return (grad_down[None], grad_hidden[None], grad_probs)


def local(upstream, combine_weights, expert_ids, saved_hidden, down_weight):
    tokens, features = upstream.shape
    n = lax.axis_size("dp")
    outer = n // INNER
    every_token_to_both = (
        lax.axis_size("expert") == 2
        and expert_ids.shape[1] == 2
        and saved_hidden.shape[1] == 2 * tokens
        and tokens == LANES
    )
    splits = n % INNER == 0 and outer & (outer - 1) == 0 and features % (n * 16) == 0
    if every_token_to_both and splits and (features // max(outer, 1)) % LANES == 0:
        return both_experts(upstream, combine_weights, expert_ids, saved_hidden, down_weight)
    return any_experts(upstream, combine_weights, expert_ids, saved_hidden, down_weight)


def solution(mesh):
    return jax.shard_map(
        local,
        mesh=mesh,
        in_specs=(
            P(("expert", "dp"), None),
            P(("expert", "dp"), None),
            P(("expert", "dp"), None),
            P("expert", "dp", None),
            P("expert", None, None),
        ),
        out_specs=(P("expert", "dp", None), P("expert", "dp", None), P(("expert", "dp"), None)),
        check_vma=False,
    )
```

```python
import functools

import jax
import jax.numpy as jnp
from jax import lax
from jax.experimental import pallas as pl
from jax.experimental.pallas import tpu as pltpu
from jax.sharding import PartitionSpec as P

INNER = 4
LANES = 128
VMEM = pl.BlockSpec(memory_space=pltpu.VMEM)
HBM = pl.BlockSpec(memory_space=pltpu.HBM)
LOAD = pl.BlockSpec(memory_space=pltpu.VMEM)
ANY = pl.BlockSpec(memory_space=pl.ANY)
TURNED = (((1,), (1,)), ((), ()))


def contract_rows(left_rows, right_rows):
    return lax.dot_general(
        left_rows, right_rows, (((0,), (0,)), ((), ())), preferred_element_type=jnp.float32
    )


def after(value, *others):
    return lax.optimization_barrier((value, *others))[0]


def call(*jobs, waits=(), vmem=8, cost=0):
    specs = [spec for job in jobs for spec in job[4] or [VMEM] * len(job[1])]
    args = [arg for job in jobs for arg in job[1]]
    outs = tuple(jax.ShapeDtypeStruct(*out) for job in jobs for out in job[2])
    scratch = [item for job in jobs for item in job[3]]

    def body(*refs):
        ins, rest = refs[: len(args)], refs[len(args) + len(waits) :]
        out_refs, temps = rest[: len(outs)], rest[len(outs) :]
        for kernel, job_args, job_outs, job_scratch, _ in jobs:
            x, y, z = len(job_args), len(job_outs), len(job_scratch)
            kernel(*ins[:x], *out_refs[:y], *temps[:z])
            ins, out_refs, temps = ins[x:], out_refs[y:], temps[z:]

    place = lambda arg, spec: arg if spec is VMEM else pltpu.with_memory_space_constraint(arg, pltpu.HBM)
    return pl.pallas_call(
        body,
        out_shape=outs,
        in_specs=specs + [ANY] * len(waits),
        out_specs=tuple(VMEM for _ in outs),
        scratch_shapes=scratch,
        compiler_params=pltpu.CompilerParams(vmem_limit_bytes=vmem << 20),
        cost_estimate=pl.CostEstimate(flops=cost, bytes_accessed=cost, transcendentals=0),
    )(*[place(*pair) for pair in zip(args, specs)], *waits)


def chunk_start(k, chunk):
    group = lax.axis_index("dp") // INNER
    return pl.multiple_of((group ^ k) * chunk, LANES)


def prepare_kernel(outer, chunk, up_hbm, hidden_hbm, ids_ref, weights_ref, *refs):
    first_ref, column_ref, act_refs = refs[0], refs[1], refs[2:4]
    own_refs, send_refs = refs[4 : 4 + outer], refs[4 + outer : -3]
    up_ref, hidden_ref, sems = refs[-3:]
    top = outer - 1
    loads = []
    for k in range(outer):
        cols = pl.ds(chunk_start(k, chunk), chunk)
        loads.append(pltpu.make_async_copy(up_hbm.at[:, cols], up_ref.at[k], sems.at[k]))
    loads.append(pltpu.make_async_copy(hidden_hbm, hidden_ref, sems.at[outer]))
    for k in [top, outer] + list(range(top - 1, -1, -1)):
        loads[k].start()
    expert = lax.axis_index("expert")

    def token_weight(of):
        picked = jnp.where(ids_ref[...] == of, weights_ref[...].astype(jnp.float32), 0.0)
        lanes = jnp.sum(picked, axis=0, keepdims=True)
        return jnp.broadcast_to(lanes, (LANES, lanes.shape[1])).T

    weight = token_weight(expert)
    column_ref[...] = weight
    weight = weight[:, :1]
    first_ref[:, chunk:] = token_weight(1 - expert).astype(jnp.bfloat16)
    for k in range(top, -1, -1):
        loads[k].wait()
        rows = up_ref[k]
        (send_refs[k] if k < top else first_ref)[:, :chunk] = rows
        own_refs[k][...] = (weight * rows.astype(jnp.float32)).astype(jnp.bfloat16).T
    loads[outer].wait()
    half, hidden_units = hidden_ref.shape[0] // 2, hidden_ref.shape[1] // 2
    for part in range(2):
        source = pl.ds(pl.multiple_of((expert ^ part) * half, half), half)
        for start, out_ref in zip((0, act_refs[0].shape[1]), act_refs):
            stop = start + out_ref.shape[1]
            gate = hidden_ref[source, start:stop].astype(jnp.float32)
            up = hidden_ref[source, hidden_units + start : hidden_units + stop].astype(jnp.float32)
            act = gate * jax.nn.sigmoid(gate) * up
            out_ref[part * half : (part + 1) * half, :] = act.astype(jnp.bfloat16)


def split_kernel(chunk, got_ref, first_ref, own_ref, *refs):
    pays, scaled_ref = refs[:-1], refs[-1]
    weight = first_ref[:, chunk : chunk + 1].astype(jnp.float32)
    scaled = (weight * got_ref[:, :chunk].astype(jnp.float32)).astype(jnp.bfloat16)
    scaled_ref[...] = scaled.T
    piece = chunk // INNER
    mine = lax.axis_index("dp") % INNER
    for j in range(INNER):
        rows = pl.ds(pl.multiple_of((mine ^ j) * piece, 16), piece)
        pays[j][:, :LANES] = own_ref[rows, :]
        pays[j][:, LANES:] = scaled_ref[rows, :]


def partial_kernel(*refs):
    pays, acts, adds, out_ref = refs[:INNER], refs[INNER : 2 * INNER], refs[2 * INNER : -1], refs[-1]
    total = None
    for pay, act in zip(pays, acts):
        term = jnp.dot(pay[...], act[...], preferred_element_type=jnp.float32)
        total = term if total is None else total + term
    for add in adds:
        total = total + add[...].astype(jnp.float32)
    out_ref[...] = total.astype(out_ref.dtype)


def whole_kernel(*refs):
    pays, acts, out_ref = refs[:INNER], refs[INNER : 3 * INNER], refs[-1]
    start = 0
    for part in (acts[:INNER], acts[INNER:]):
        stop = start + part[0].shape[1]
        partial_kernel(*pays, *part, out_ref.at[:, start:stop])
        start = stop


def final_kernel(base_ref, side_ref, left_ref, right_ref, out_ref):
    split = left_ref.shape[1]
    for cols, ref in ((slice(0, split), left_ref), (slice(split, None), right_ref)):
        both = side_ref[:, cols].astype(jnp.float32) + ref[...].astype(jnp.float32)
        out_ref[:, cols] = base_ref[:, cols] + both


def probs_kernel(ids_ref, own_ref, back_ref, out_ref):
    mine = ids_ref[...] == lax.axis_index("expert")
    out_ref[...] = jnp.where(mine, own_ref[:1], back_ref[:1])


def hidden_kernel(outer, chunk, column_ref, up_hbm, hidden_hbm, w_hbm, *refs):
    got_refs = refs[:outer]
    out_ref, own_score, got_score = refs[outer : outer + 3]
    routed_ref, hidden_ref, w_ref, sems = refs[outer + 3 :]
    tokens = up_hbm.shape[0]
    hidden_units = w_ref.shape[0]
    width = 2 * LANES
    blocks = hidden_units // width
    expert = lax.axis_index("expert")
    top = pltpu.make_async_copy(up_hbm, routed_ref.at[pl.ds(0, tokens)], sems.at[blocks])
    stored = pltpu.make_async_copy(hidden_hbm, hidden_ref, sems.at[blocks + 1])
    loads = []
    for i in range(blocks):
        rows = pl.ds(i * width, width)
        loads.append(pltpu.make_async_copy(w_hbm.at[rows], w_ref.at[rows], sems.at[i]))
    top.start()
    loads[0].start()
    stored.start()
    for load in loads[1:]:
        load.start()
    for k in range(outer):
        routed_ref[tokens:, pl.ds(chunk_start(k, chunk), chunk)] = got_refs[k][:, :chunk]
    weights = [column_ref[:, :1], got_refs[outer - 1][:, chunk : chunk + 1].astype(jnp.float32)]
    scores = [None, None]
    top.wait()
    for i in range(blocks):
        loads[i].wait()
        backward = lax.dot_general(
            routed_ref[...], w_ref[i * width : (i + 1) * width, :], TURNED, preferred_element_type=jnp.float32
        )
        if i == 0:
            stored.wait()
        gate_cols = slice(i * width, (i + 1) * width)
        up_cols = slice(hidden_units + i * width, hidden_units + (i + 1) * width)
        for part in range(2):
            back = backward[part * tokens : (part + 1) * tokens]
            rows = pl.ds(pl.multiple_of((expert ^ part) * tokens, tokens), tokens)
            gate = hidden_ref[rows, gate_cols].astype(jnp.float32)
            up = hidden_ref[rows, up_cols].astype(jnp.float32)
            sig = jax.nn.sigmoid(gate)
            act = (gate * sig * up).astype(jnp.bfloat16).astype(jnp.float32)
            score = jnp.sum(back * act, axis=1, keepdims=True)
            scores[part] = score if i == 0 else scores[part] + score
            grad = weights[part] * back
            out_ref[rows, gate_cols] = (grad * up * sig * (1.0 + gate * (1.0 - sig))).astype(jnp.bfloat16)
            out_ref[rows, up_cols] = (grad * gate * sig).astype(jnp.bfloat16)
    for score, ref in zip(scores, (own_score, got_score)):
        ref[...] = jnp.broadcast_to(score, (tokens, LANES)).T[:8]


def both_experts(upstream, combine_weights, expert_ids, saved_hidden, down_weight):
    tokens, features = upstream.shape
    n = lax.axis_size("dp")
    outer = n // INNER
    chunk, piece = features // outer, features // n
    hidden_units = down_weight.shape[1]
    stored, weights = saved_hidden[0], down_weight[0]
    ids, combine = expert_ids.T, combine_weights.T
    flip = [(0, 1), (1, 0)]
    cross = lambda value: lax.ppermute(value, "expert", flip)
    swap = lambda value, bit: lax.ppermute(value, "dp", [(i, i ^ bit) for i in range(n)])
    rows = stored.shape[0]
    widths = (hidden_units // 2, hidden_units // 2)
    bf16, f32 = jnp.bfloat16, jnp.float32

    prepared = call((
        functools.partial(prepare_kernel, outer, chunk),
        [upstream, stored, ids, combine],
        [((tokens, chunk + LANES), bf16), ((tokens, LANES), f32)]
        + [((rows, width), bf16) for width in widths]
        + [((chunk, tokens), bf16)] * outer
        + [((tokens, chunk), bf16)] * (outer - 1),
        [
            pltpu.VMEM((outer, tokens, chunk), bf16),
            pltpu.VMEM((rows, 2 * hidden_units), bf16),
            pltpu.SemaphoreType.DMA((outer + 1,)),
        ],
        [HBM, HBM, LOAD, LOAD],
    ))
    first, column, mine = prepared[0], prepared[1], prepared[2:4]
    own, send = prepared[4 : 4 + outer], prepared[4 + outer :]

    def split(k):
        shapes = [((piece, 2 * tokens), bf16)] * INNER
        scratch = [pltpu.VMEM((chunk, tokens), bf16)]
        return functools.partial(split_kernel, chunk), [got[k], got[3], own[k]], shapes, scratch, None

    def spread(pays):
        return [pays[0]] + [swap(pays[j], j) for j in range(1, INNER)]

    def partial(pays, h, *adds):
        sides = [acts[h][j] for j in range(INNER)]
        return partial_kernel, [*pays, *sides, *adds], [((piece, widths[h]), bf16)], [], None

    def whole(pays, kind):
        sides = [acts[h][j] for h in range(2) for j in range(INNER)]
        return whole_kernel, [*pays, *sides], [((piece, hidden_units), kind)], [], None

    got = {3: cross(first)}
    acts = [{0: mine[h], 1: swap(mine[h], 1), 2: swap(mine[h], 2)} for h in range(2)]
    pays = {}
    cut = call(split(3))
    pays[3] = spread(cut)
    got[2] = cross(after(send[2], cut[0]))
    acts[0][3] = swap(after(acts[0][2], cut[0]), 1)
    acts[1][3] = swap(after(acts[1][2], acts[0][3]), 1)
    far0, *cut = call(partial(pays[3], 0), split(2))
    near0 = swap(far0, INNER)
    pays[2] = spread(cut)
    got[1] = cross(after(send[1], cut[0]))
    far1, = call(partial(pays[3], 1), waits=(far0,))
    near1 = swap(far1, INNER)
    wide0, *cut = call(partial(pays[2], 0, near0), split(1), waits=(far1,))
    last0 = swap(wide0, 2 * INNER)
    pays[1] = spread(cut)
    got[0] = cross(after(send[0], cut[0]))
    wide1, = call(partial(pays[2], 1, near1), waits=(wide0,))
    last1 = swap(wide1, 2 * INNER)
    side, *cut = call(whole(pays[1], bf16), split(0), waits=(wide1,))
    pays[0] = spread(cut)

    grad_hidden, own_score, got_score = call(
        (
            functools.partial(hidden_kernel, outer, chunk),
            [column, upstream, stored, weights, *[got[k] for k in range(outer)]],
            [(stored.shape, bf16), ((8, tokens), f32), ((8, tokens), f32)],
            [
                pltpu.VMEM((rows, features), bf16),
                pltpu.VMEM(stored.shape, bf16),
                pltpu.VMEM(weights.shape, bf16),
                pltpu.SemaphoreType.DMA((hidden_units // (2 * LANES) + 2,)),
            ],
            [VMEM, HBM, HBM, HBM] + [VMEM] * outer,
        ),
        waits=(side,), vmem=18,
    )
    side = swap(side, INNER)
    back_score = cross(got_score)
    base, = call(whole(pays[0], f32), waits=(own_score,))
    grad_probs, = call((probs_kernel, [ids, own_score, back_score], [(ids.shape, f32)], [], None))
    grad_down, = call((final_kernel, [base, side, last0, last1], [((piece, hidden_units), f32)], [], None))
    return grad_down[None], grad_hidden[None], grad_probs.T


def any_experts(upstream, combine_weights, expert_ids, saved_hidden, down_weight):
    tok_rows, features = upstream.shape
    experts = lax.axis_size("expert")
    hidden_units = down_weight.shape[1]
    capacity = saved_hidden.shape[1] // experts
    labels = lax.broadcasted_iota(jnp.int32, (1, 1, experts), 2)
    matched = expert_ids[:, :, None] == labels
    member = jnp.sum(matched.astype(jnp.int32), axis=1)
    slot_rank = jnp.cumsum(member, axis=0) - member
    token_iota = lax.broadcasted_iota(jnp.int32, (tok_rows, experts, capacity), 0)
    slot_iota = lax.broadcasted_iota(jnp.int32, (tok_rows, experts, capacity), 2)
    placed = (member[:, :, None] == 1) & (slot_rank[:, :, None] == slot_iota)
    source = jnp.sum(jnp.where(placed, token_iota, 0), axis=0)
    filled = jnp.any(placed, axis=0)
    token_weight = jnp.sum(
        jnp.where(matched, combine_weights[:, :, None].astype(jnp.float32), 0.0), axis=1
    )
    send_rows = jnp.where(filled[:, :, None], upstream[source], jnp.zeros((), jnp.bfloat16))
    send_weight = jnp.where(
        filled, jnp.take_along_axis(token_weight.T, source, axis=1), 0.0
    ).astype(jnp.bfloat16)
    got_rows, got_weight = (
        lax.all_to_all(send_rows, "expert", split_axis=0, concat_axis=0, tiled=True),
        lax.all_to_all(send_weight, "expert", split_axis=0, concat_axis=0, tiled=True),
    )
    routed = got_rows.reshape(experts * capacity, features)
    row_weight = got_weight.reshape(experts * capacity, 1).astype(jnp.float32)
    stored = saved_hidden[0]
    gate_pre = stored[:, :hidden_units].astype(jnp.float32)
    up_pre = stored[:, hidden_units:].astype(jnp.float32)
    sigmoid_gate = jax.nn.sigmoid(gate_pre)
    activated = (gate_pre * sigmoid_gate * up_pre).astype(jnp.bfloat16)
    scaled = (row_weight * routed.astype(jnp.float32)).astype(jnp.bfloat16)
    weights = down_weight[0]
    backward = lax.dot_general(
        routed, weights, (((1,), (1,)), ((), ())), preferred_element_type=jnp.float32
    )
    grad_act = row_weight * backward
    grad_gate = grad_act * up_pre * sigmoid_gate * (1.0 + gate_pre * (1.0 - sigmoid_gate))
    grad_up = grad_act * gate_pre * sigmoid_gate
    grad_hidden = jnp.concatenate([grad_gate, grad_up], axis=1).astype(jnp.bfloat16)
    outputs = jnp.dot(activated, weights, preferred_element_type=jnp.float32)
    scores = jnp.sum(routed.astype(jnp.float32) * outputs, axis=1)
    returned = lax.all_to_all(
        scores.reshape(experts, capacity), "expert", split_axis=0, concat_axis=0, tiled=True
    )
    slot_of = jnp.sum(jnp.where(matched, slot_rank[:, None, :], 0), axis=2)
    flat_index = expert_ids * capacity + slot_of
    score_table = returned.reshape(experts * capacity)
    cell_ids = lax.broadcasted_iota(jnp.int32, (1, 1, experts * capacity), 2)
    grad_probs = jnp.sum(
        jnp.where(flat_index[:, :, None] == cell_ids, score_table[None, None, :], 0.0), axis=2
    )
    grad_down = lax.psum_scatter(
        contract_rows(scaled, activated), "dp", scatter_dimension=0, tiled=True
    )
    return (grad_down[None], grad_hidden[None], grad_probs)


def local(upstream, combine_weights, expert_ids, saved_hidden, down_weight):
    tokens, features = upstream.shape
    n = lax.axis_size("dp")
    outer = n // INNER
    every_token_to_both = (
        lax.axis_size("expert") == 2
        and expert_ids.shape[1] == 2
        and saved_hidden.shape[1] == 2 * tokens
        and tokens == LANES
    )
    splits = n == 4 * INNER and features % (n * 16) == 0 and features % (outer * LANES) == 0
    hidden_units = down_weight.shape[1]
    if every_token_to_both and splits and hidden_units % (4 * LANES) == 0:
        return both_experts(upstream, combine_weights, expert_ids, saved_hidden, down_weight)
    return any_experts(upstream, combine_weights, expert_ids, saved_hidden, down_weight)


def solution(mesh):
    return jax.shard_map(
        local,
        mesh=mesh,
        in_specs=(
            P(("expert", "dp"), None),
            P(("expert", "dp"), None),
            P(("expert", "dp"), None),
            P("expert", "dp", None),
            P("expert", None, None),
        ),
        out_specs=(P("expert", "dp", None), P("expert", "dp", None), P(("expert", "dp"), None)),
        check_vma=False,
    )
```

```python
import functools

import jax
import jax.numpy as jnp
from jax import lax
from jax.experimental import pallas as pl
from jax.experimental.pallas import tpu as pltpu
from jax.sharding import PartitionSpec as P

INNER = 4
LANES = 128
VMEM = pl.BlockSpec(memory_space=pltpu.VMEM)
HBM = pl.BlockSpec(memory_space=pltpu.HBM)
LOAD = pl.BlockSpec(memory_space=pltpu.VMEM)
ANY = pl.BlockSpec(memory_space=pl.ANY)
TURNED = (((1,), (1,)), ((), ()))


def contract_rows(left_rows, right_rows):
    return lax.dot_general(
        left_rows, right_rows, (((0,), (0,)), ((), ())), preferred_element_type=jnp.float32
    )


def after(value, *others):
    return lax.optimization_barrier((value, *others))[0]


def call(*jobs, waits=(), vmem=8):
    specs = [spec for job in jobs for spec in job[4] or [VMEM] * len(job[1])]
    args = [arg for job in jobs for arg in job[1]]
    outs = tuple(jax.ShapeDtypeStruct(*out) for job in jobs for out in job[2])
    scratch = [item for job in jobs for item in job[3]]

    def body(*refs):
        ins, rest = refs[: len(args)], refs[len(args) + len(waits) :]
        out_refs, temps = rest[: len(outs)], rest[len(outs) :]
        for kernel, job_args, job_outs, job_scratch, _ in jobs:
            x, y, z = len(job_args), len(job_outs), len(job_scratch)
            kernel(*ins[:x], *out_refs[:y], *temps[:z])
            ins, out_refs, temps = ins[x:], out_refs[y:], temps[z:]

    place = lambda arg, spec: arg if spec is VMEM else pltpu.with_memory_space_constraint(arg, pltpu.HBM)
    return pl.pallas_call(
        body,
        out_shape=outs,
        in_specs=specs + [ANY] * len(waits),
        out_specs=tuple(VMEM for _ in outs),
        scratch_shapes=scratch,
        compiler_params=pltpu.CompilerParams(vmem_limit_bytes=vmem << 20),
    )(*[place(*pair) for pair in zip(args, specs)], *waits)


def chunk_start(k, chunk):
    group = lax.axis_index("dp") // INNER
    return pl.multiple_of((group ^ k) * chunk, LANES)


def prepare_kernel(pairs, chunk, up_hbm, hidden_hbm, ids_ref, weights_ref, *refs):
    send_refs, column_ref, act_refs = refs[: len(pairs)], refs[len(pairs)], refs[len(pairs) + 1 : len(pairs) + 3]
    own_refs = refs[len(pairs) + 3 : -3]
    up_ref, hidden_ref, sems = refs[-3:]
    order = [k for pair in pairs for k in pair]
    outer = len(order)
    loads = {}
    for k in order:
        cols = pl.ds(chunk_start(k, chunk), chunk)
        loads[k] = pltpu.make_async_copy(up_hbm.at[:, cols], up_ref.at[k], sems.at[k])
        loads[k].start()
    stored = pltpu.make_async_copy(hidden_hbm, hidden_ref, sems.at[outer])
    stored.start()
    expert = lax.axis_index("expert")

    def token_weight(of):
        picked = jnp.where(ids_ref[...] == of, weights_ref[...].astype(jnp.float32), 0.0)
        lanes = jnp.sum(picked, axis=0, keepdims=True)
        return jnp.broadcast_to(lanes, (LANES, lanes.shape[1])).T

    weight = token_weight(expert)
    column_ref[...] = weight
    weight = weight[:, :1]
    send_refs[0][:, len(pairs[0]) * chunk :] = token_weight(1 - expert).astype(jnp.bfloat16)
    for send_ref, pair in zip(send_refs, pairs):
        for i, k in enumerate(pair):
            loads[k].wait()
            rows = up_ref[k]
            send_ref[:, i * chunk : (i + 1) * chunk] = rows
            own_refs[order.index(k)][...] = (weight * rows.astype(jnp.float32)).astype(jnp.bfloat16).T
    stored.wait()
    half, hidden_units = hidden_ref.shape[0] // 2, hidden_ref.shape[1] // 2
    for part in range(2):
        source = pl.ds(pl.multiple_of((expert ^ part) * half, half), half)
        gate = hidden_ref[source, :hidden_units].astype(jnp.float32)
        up = hidden_ref[source, hidden_units:].astype(jnp.float32)
        act = (gate * jax.nn.sigmoid(gate) * up).astype(jnp.bfloat16)
        for i, act_ref in enumerate(act_refs):
            width = act_ref.shape[1]
            act_ref[part * half : (part + 1) * half, :] = act[:, i * width : (i + 1) * width]


def split_kernel(chunk, got_ref, first_ref, *refs):
    owns, pays, scaled_ref = refs[: -INNER - 1], refs[-INNER - 1 : -1], refs[-1]
    column = first_ref.shape[1] - LANES
    weight = first_ref[:, column : column + 1].astype(jnp.float32)
    piece = chunk // INNER
    mine = lax.axis_index("dp") % INNER
    for i, own_ref in enumerate(owns):
        scaled = weight * got_ref[:, i * chunk : (i + 1) * chunk].astype(jnp.float32)
        scaled_ref[...] = scaled.astype(jnp.bfloat16).T
        for j in range(INNER):
            rows = pl.ds(pl.multiple_of((mine ^ j) * piece, 16), piece)
            pays[j][i * piece : (i + 1) * piece, :LANES] = own_ref[rows, :]
            pays[j][i * piece : (i + 1) * piece, LANES:] = scaled_ref[rows, :]


def parts_kernel(adds, *refs):
    pays, acts, rest = refs[:INNER], refs[INNER : 3 * INNER], refs[3 * INNER :]
    adds, outs = rest[:adds], rest[adds:]
    total = []
    for half in (acts[:INNER], acts[INNER:]):
        terms = [jnp.dot(p[...], a[...], preferred_element_type=jnp.float32) for p, a in zip(pays, half)]
        total.append(functools.reduce(jnp.add, terms))
    total = jnp.concatenate(total, axis=1)
    for add in adds:
        total = total + add[...].astype(jnp.float32)
    start = 0
    for out_ref in outs:
        stop = start + out_ref.shape[1]
        out_ref[...] = total[:, start:stop].astype(out_ref.dtype)
        start = stop


def final_kernel(sides, base_ref, *refs):
    terms, out_ref = refs[:-1], refs[-1]
    side, last = [
        jnp.concatenate([ref[...].astype(jnp.float32) for ref in part], axis=1)
        for part in (terms[:sides], terms[sides:])
    ]
    out_ref[...] = base_ref[...] + (side + last)


def probs_kernel(ids_ref, own_ref, back_ref, out_ref):
    mine = ids_ref[...] == lax.axis_index("expert")
    out_ref[...] = jnp.where(mine, own_ref[:1], back_ref[:1])


def hidden_kernel(pairs, chunk, column_ref, up_hbm, hidden_hbm, w_hbm, *refs):
    got_refs = refs[: len(pairs)]
    out_ref, own_score, got_score = refs[len(pairs) : len(pairs) + 3]
    routed_ref, hidden_ref, w_ref, sems = refs[len(pairs) + 3 :]
    tokens = up_hbm.shape[0]
    hidden_units = w_ref.shape[0]
    width = 2 * LANES
    blocks = hidden_units // width
    expert = lax.axis_index("expert")
    top = pltpu.make_async_copy(up_hbm, routed_ref.at[pl.ds(0, tokens)], sems.at[blocks])
    stored = pltpu.make_async_copy(hidden_hbm, hidden_ref, sems.at[blocks + 1])
    loads = []
    for i in range(blocks):
        rows = pl.ds(i * width, width)
        loads.append(pltpu.make_async_copy(w_hbm.at[rows], w_ref.at[rows], sems.at[i]))
    top.start()
    loads[0].start()
    stored.start()
    for load in loads[1:]:
        load.start()
    for got_ref, pair in zip(got_refs, pairs):
        for i, k in enumerate(pair):
            routed_ref[tokens:, pl.ds(chunk_start(k, chunk), chunk)] = got_ref[:, i * chunk : (i + 1) * chunk]
    column = len(pairs[0]) * chunk
    weights = [column_ref[:, :1], got_refs[0][:, column : column + 1].astype(jnp.float32)]
    scores = [None, None]
    top.wait()
    for i in range(blocks):
        loads[i].wait()
        backward = lax.dot_general(
            routed_ref[...], w_ref[i * width : (i + 1) * width, :], TURNED, preferred_element_type=jnp.float32
        )
        if i == 0:
            stored.wait()
        gate_cols = slice(i * width, (i + 1) * width)
        up_cols = slice(hidden_units + i * width, hidden_units + (i + 1) * width)
        for part in range(2):
            back = backward[part * tokens : (part + 1) * tokens]
            rows = pl.ds(pl.multiple_of((expert ^ part) * tokens, tokens), tokens)
            gate = hidden_ref[rows, gate_cols].astype(jnp.float32)
            up = hidden_ref[rows, up_cols].astype(jnp.float32)
            sig = jax.nn.sigmoid(gate)
            act = (gate * sig * up).astype(jnp.bfloat16).astype(jnp.float32)
            score = jnp.sum(back * act, axis=1, keepdims=True)
            scores[part] = score if i == 0 else scores[part] + score
            grad = weights[part] * back
            out_ref[rows, gate_cols] = (grad * up * sig * (1.0 + gate * (1.0 - sig))).astype(jnp.bfloat16)
            out_ref[rows, up_cols] = (grad * gate * sig).astype(jnp.bfloat16)
    for score, ref in zip(scores, (own_score, got_score)):
        ref[...] = jnp.broadcast_to(score, (tokens, LANES)).T[:8]


def both_experts(upstream, combine_weights, expert_ids, saved_hidden, down_weight):
    tokens, features = upstream.shape
    n = lax.axis_size("dp")
    outer = n // INNER
    chunk, piece = features // outer, features // n
    hidden_units = down_weight.shape[1]
    stored, weights = saved_hidden[0], down_weight[0]
    ids, combine = expert_ids.T, combine_weights.T
    flip = [(0, 1), (1, 0)]
    cross = lambda value: lax.ppermute(value, "expert", flip)
    swap = lambda value, bit: lax.ppermute(value, "dp", [(i, i ^ bit) for i in range(n)])
    rows = stored.shape[0]
    bf16, f32 = jnp.bfloat16, jnp.float32
    pairs = ((3,), (2,), (1,), (0,))
    sides = (hidden_units,)

    prepared = call((
        functools.partial(prepare_kernel, pairs, chunk),
        [upstream, stored, ids, combine],
        [((tokens, chunk + LANES), bf16)] + [((tokens, chunk), bf16)] * 3
        + [((tokens, LANES), f32)] + [((rows, hidden_units // 2), bf16)] * 2
        + [((chunk, tokens), bf16)] * outer,
        [
            pltpu.VMEM((outer, tokens, chunk), bf16),
            pltpu.VMEM((rows, 2 * hidden_units), bf16),
            pltpu.SemaphoreType.DMA((outer + 1,)),
        ],
        [HBM, HBM, LOAD, LOAD],
    ))
    send, column = prepared[:outer], prepared[outer]
    mine, own = prepared[outer + 1 : outer + 3], prepared[outer + 3 :]

    def split_job(i):
        return (
            functools.partial(split_kernel, chunk),
            [got[i], got[0], own[i]],
            [((piece, 2 * tokens), bf16)] * INNER,
            [pltpu.VMEM((chunk, tokens), bf16)],
            None,
        )

    def spread(cut):
        return [cut[0]] + [swap(cut[j], j) for j in range(1, INNER)], cut[0]

    def split(i, *waits):
        return spread(call(split_job(i), waits=waits))

    def parts(i, kind, cuts, *adds):
        kernel = functools.partial(parts_kernel, len(adds))
        args = [*pays[i], *acts[0], *acts[1], *adds]
        return kernel, args, [((piece, width), kind) for width in cuts], [], None

    got, pays, marks = {}, {}, {}
    got[0] = cross(send[0])
    acts = [[mine[h], swap(mine[h], 1), swap(mine[h], 2)] for h in range(2)]
    pays[0], marks[0] = split(0)
    got[1] = cross(after(send[1], marks[0]))
    acts[0].append(swap(after(acts[0][2], marks[0]), 1))
    acts[1].append(swap(after(acts[1][2], acts[0][3]), 1))
    far, *cut = call(parts(0, bf16, (hidden_units,)), split_job(1))
    near = swap(far, INNER)
    pays[1], marks[1] = spread(cut)
    got[2] = cross(after(send[2], acts[0][3]))
    pays[2], marks[2] = split(2, far)
    wide, = call(parts(1, bf16, (hidden_units,), near), waits=(marks[2],))
    last = [swap(wide, 2 * INNER)]
    got[3] = cross(after(send[3], marks[2]))
    *side, _0, _1, _2, _3 = call(parts(2, bf16, sides), split_job(3), waits=(wide,))
    pays[3], marks[3] = spread((_0, _1, _2, _3))
    side = [swap(part, INNER) for part in side]

    grad_hidden, own_score, got_score = call(
        (
            functools.partial(hidden_kernel, pairs, chunk),
            [column, upstream, stored, weights, *[got[i] for i in range(outer)]],
            [(stored.shape, bf16), ((8, tokens), f32), ((8, tokens), f32)],
            [
                pltpu.VMEM((rows, features), bf16),
                pltpu.VMEM(stored.shape, bf16),
                pltpu.VMEM(weights.shape, bf16),
                pltpu.SemaphoreType.DMA((hidden_units // (2 * LANES) + 2,)),
            ],
            [VMEM, HBM, HBM, HBM] + [VMEM] * outer,
        ),
        waits=(marks[3],), vmem=18,
    )
    back_score = cross(got_score)
    base, = call(parts(3, f32, (hidden_units,)), waits=(own_score,))
    grad_probs, = call((probs_kernel, [ids, own_score, back_score], [(ids.shape, f32)], [], None), waits=last)
    grad_down, = call((
        functools.partial(final_kernel, len(side)), [base, *side, *last],
        [((piece, hidden_units), f32)], [], None,
    ))
    return grad_down[None], grad_hidden[None], grad_probs.T


def any_experts(upstream, combine_weights, expert_ids, saved_hidden, down_weight):
    tok_rows, features = upstream.shape
    experts = lax.axis_size("expert")
    hidden_units = down_weight.shape[1]
    capacity = saved_hidden.shape[1] // experts
    labels = lax.broadcasted_iota(jnp.int32, (1, 1, experts), 2)
    matched = expert_ids[:, :, None] == labels
    member = jnp.sum(matched.astype(jnp.int32), axis=1)
    slot_rank = jnp.cumsum(member, axis=0) - member
    token_iota = lax.broadcasted_iota(jnp.int32, (tok_rows, experts, capacity), 0)
    slot_iota = lax.broadcasted_iota(jnp.int32, (tok_rows, experts, capacity), 2)
    placed = (member[:, :, None] == 1) & (slot_rank[:, :, None] == slot_iota)
    source = jnp.sum(jnp.where(placed, token_iota, 0), axis=0)
    filled = jnp.any(placed, axis=0)
    token_weight = jnp.sum(
        jnp.where(matched, combine_weights[:, :, None].astype(jnp.float32), 0.0), axis=1
    )
    send_rows = jnp.where(filled[:, :, None], upstream[source], jnp.zeros((), jnp.bfloat16))
    send_weight = jnp.where(
        filled, jnp.take_along_axis(token_weight.T, source, axis=1), 0.0
    ).astype(jnp.bfloat16)
    got_rows, got_weight = (
        lax.all_to_all(send_rows, "expert", split_axis=0, concat_axis=0, tiled=True),
        lax.all_to_all(send_weight, "expert", split_axis=0, concat_axis=0, tiled=True),
    )
    routed = got_rows.reshape(experts * capacity, features)
    row_weight = got_weight.reshape(experts * capacity, 1).astype(jnp.float32)
    stored = saved_hidden[0]
    gate_pre = stored[:, :hidden_units].astype(jnp.float32)
    up_pre = stored[:, hidden_units:].astype(jnp.float32)
    sigmoid_gate = jax.nn.sigmoid(gate_pre)
    activated = (gate_pre * sigmoid_gate * up_pre).astype(jnp.bfloat16)
    scaled = (row_weight * routed.astype(jnp.float32)).astype(jnp.bfloat16)
    weights = down_weight[0]
    backward = lax.dot_general(
        routed, weights, (((1,), (1,)), ((), ())), preferred_element_type=jnp.float32
    )
    grad_act = row_weight * backward
    grad_gate = grad_act * up_pre * sigmoid_gate * (1.0 + gate_pre * (1.0 - sigmoid_gate))
    grad_up = grad_act * gate_pre * sigmoid_gate
    grad_hidden = jnp.concatenate([grad_gate, grad_up], axis=1).astype(jnp.bfloat16)
    outputs = jnp.dot(activated, weights, preferred_element_type=jnp.float32)
    scores = jnp.sum(routed.astype(jnp.float32) * outputs, axis=1)
    returned = lax.all_to_all(
        scores.reshape(experts, capacity), "expert", split_axis=0, concat_axis=0, tiled=True
    )
    slot_of = jnp.sum(jnp.where(matched, slot_rank[:, None, :], 0), axis=2)
    flat_index = expert_ids * capacity + slot_of
    score_table = returned.reshape(experts * capacity)
    cell_ids = lax.broadcasted_iota(jnp.int32, (1, 1, experts * capacity), 2)
    grad_probs = jnp.sum(
        jnp.where(flat_index[:, :, None] == cell_ids, score_table[None, None, :], 0.0), axis=2
    )
    grad_down = lax.psum_scatter(
        contract_rows(scaled, activated), "dp", scatter_dimension=0, tiled=True
    )
    return (grad_down[None], grad_hidden[None], grad_probs)


def local(upstream, combine_weights, expert_ids, saved_hidden, down_weight):
    tokens, features = upstream.shape
    n = lax.axis_size("dp")
    outer = n // INNER
    every_token_to_both = (
        lax.axis_size("expert") == 2
        and expert_ids.shape[1] == 2
        and saved_hidden.shape[1] == 2 * tokens
        and tokens == LANES
    )
    splits = n == 4 * INNER and features % (n * 16) == 0 and features % (outer * LANES) == 0
    hidden_units = down_weight.shape[1]
    if every_token_to_both and splits and hidden_units % (4 * LANES) == 0:
        return both_experts(upstream, combine_weights, expert_ids, saved_hidden, down_weight)
    return any_experts(upstream, combine_weights, expert_ids, saved_hidden, down_weight)


def solution(mesh):
    return jax.shard_map(
        local,
        mesh=mesh,
        in_specs=(
            P(("expert", "dp"), None),
            P(("expert", "dp"), None),
            P(("expert", "dp"), None),
            P("expert", "dp", None),
            P("expert", None, None),
        ),
        out_specs=(P("expert", "dp", None), P("expert", "dp", None), P(("expert", "dp"), None)),
        check_vma=False,
    )
```

```python
import functools

import jax
import jax.numpy as jnp
from jax import lax
from jax.experimental import pallas as pl
from jax.experimental.pallas import tpu as pltpu
from jax.sharding import PartitionSpec as P

INNER = 4
LANES = 128
VMEM = pl.BlockSpec(memory_space=pltpu.VMEM)
HBM = pl.BlockSpec(memory_space=pltpu.HBM)
LOAD = pl.BlockSpec(memory_space=pltpu.VMEM)
ANY = pl.BlockSpec(memory_space=pl.ANY)
TURNED = (((1,), (1,)), ((), ()))


def contract_rows(left_rows, right_rows):
    return lax.dot_general(
        left_rows, right_rows, (((0,), (0,)), ((), ())), preferred_element_type=jnp.float32
    )


def after(value, *others):
    return lax.optimization_barrier((value, *others))[0]


def call(*jobs, waits=(), vmem=8):
    specs = [spec for job in jobs for spec in job[4] or [VMEM] * len(job[1])]
    args = [arg for job in jobs for arg in job[1]]
    outs = tuple(jax.ShapeDtypeStruct(*out) for job in jobs for out in job[2])
    scratch = [item for job in jobs for item in job[3]]

    def body(*refs):
        ins, rest = refs[: len(args)], refs[len(args) + len(waits) :]
        out_refs, temps = rest[: len(outs)], rest[len(outs) :]
        for kernel, job_args, job_outs, job_scratch, _ in jobs:
            x, y, z = len(job_args), len(job_outs), len(job_scratch)
            kernel(*ins[:x], *out_refs[:y], *temps[:z])
            ins, out_refs, temps = ins[x:], out_refs[y:], temps[z:]

    place = lambda arg, spec: arg if spec is VMEM else pltpu.with_memory_space_constraint(arg, pltpu.HBM)
    return pl.pallas_call(
        body,
        out_shape=outs,
        in_specs=specs + [ANY] * len(waits),
        out_specs=tuple(VMEM for _ in outs),
        scratch_shapes=scratch,
        compiler_params=pltpu.CompilerParams(vmem_limit_bytes=vmem << 20),
    )(*[place(*pair) for pair in zip(args, specs)], *waits)


def chunk_start(k, chunk):
    group = lax.axis_index("dp") // INNER
    return pl.multiple_of((group ^ k) * chunk, LANES)


def token_weight(ids_ref, weights_ref, expert):
    picked = jnp.where(ids_ref[...] == expert, weights_ref[...].astype(jnp.float32), 0.0)
    lanes = jnp.sum(picked, axis=0, keepdims=True)
    return jnp.broadcast_to(lanes, (LANES, lanes.shape[1])).T


def first_kernel(k, chunk, up_hbm, hidden_hbm, ids_ref, weights_ref, send_ref, act0_ref, act1_ref, hidden_ref, sems):
    cols = pl.ds(chunk_start(k, chunk), chunk)
    rows = pltpu.make_async_copy(up_hbm.at[:, cols], send_ref.at[:, pl.ds(0, chunk)], sems.at[0])
    half, hidden_units = hidden_ref.shape[0] // 2, hidden_ref.shape[1] // 2
    loads = []
    for part in range(2):
        span = pl.ds(part * half, half)
        loads.append(pltpu.make_async_copy(hidden_hbm.at[span], hidden_ref.at[span], sems.at[1 + part]))
    for load in loads:
        load.start()
    rows.start()
    expert = lax.axis_index("expert")
    send_ref[:, chunk:] = token_weight(ids_ref, weights_ref, 1 - expert).astype(jnp.bfloat16)
    for part in range(2):
        loads[part].wait()
        target = pl.ds(pl.multiple_of((expert ^ part) * half, half), half)
        gate = hidden_ref[part * half : (part + 1) * half, :hidden_units].astype(jnp.float32)
        up = hidden_ref[part * half : (part + 1) * half, hidden_units:].astype(jnp.float32)
        act = (gate * jax.nn.sigmoid(gate) * up).astype(jnp.bfloat16)
        for i, act_ref in enumerate((act0_ref, act1_ref)):
            width = act_ref.shape[1]
            act_ref[target, :] = act[:, i * width : (i + 1) * width]
    rows.wait()


def own_kernel(order, chunk, up_hbm, ids_ref, weights_ref, *refs):
    column_ref, refs = refs[0], refs[1:]
    own_refs, send_refs = refs[: len(order)], refs[len(order) : -2]
    up_ref, sems = refs[-2:]
    loads = []
    for i, k in enumerate(order):
        cols = pl.ds(chunk_start(k, chunk), chunk)
        loads.append(pltpu.make_async_copy(up_hbm.at[:, cols], up_ref.at[i], sems.at[i]))
        loads[i].start()
    weight = token_weight(ids_ref, weights_ref, lax.axis_index("expert"))
    column_ref[...] = weight
    weight = weight[:, :1]
    for i in range(len(order)):
        loads[i].wait()
        rows = up_ref[i]
        if i:
            send_refs[i - 1][...] = rows
        own_refs[i][...] = (weight * rows.astype(jnp.float32)).astype(jnp.bfloat16).T


def split_kernel(chunk, got_ref, first_ref, *refs):
    owns, pays, scaled_ref = refs[: -INNER - 1], refs[-INNER - 1 : -1], refs[-1]
    column = first_ref.shape[1] - LANES
    weight = first_ref[:, column : column + 1].astype(jnp.float32)
    piece = chunk // INNER
    mine = lax.axis_index("dp") % INNER
    for i, own_ref in enumerate(owns):
        scaled = weight * got_ref[:, i * chunk : (i + 1) * chunk].astype(jnp.float32)
        scaled_ref[...] = scaled.astype(jnp.bfloat16).T
        for j in range(INNER):
            rows = pl.ds(pl.multiple_of((mine ^ j) * piece, 16), piece)
            pays[j][i * piece : (i + 1) * piece, :LANES] = own_ref[rows, :]
            pays[j][i * piece : (i + 1) * piece, LANES:] = scaled_ref[rows, :]


def parts_kernel(adds, *refs):
    pays, acts, rest = refs[:INNER], refs[INNER : 3 * INNER], refs[3 * INNER :]
    adds, outs = rest[:adds], rest[adds:]
    total = []
    for half in (acts[:INNER], acts[INNER:]):
        terms = [jnp.dot(p[...], a[...], preferred_element_type=jnp.float32) for p, a in zip(pays, half)]
        total.append(functools.reduce(jnp.add, terms))
    total = jnp.concatenate(total, axis=1)
    for add in adds:
        total = total + add[...].astype(jnp.float32)
    start = 0
    for out_ref in outs:
        stop = start + out_ref.shape[1]
        out_ref[...] = total[:, start:stop].astype(out_ref.dtype)
        start = stop


def final_kernel(sides, base_ref, *refs):
    terms, out_ref = refs[:-1], refs[-1]
    side, last = [
        jnp.concatenate([ref[...].astype(jnp.float32) for ref in part], axis=1)
        for part in (terms[:sides], terms[sides:])
    ]
    out_ref[...] = base_ref[...] + (side + last)


def probs_kernel(ids_ref, own_ref, back_ref, out_ref):
    mine = ids_ref[...] == lax.axis_index("expert")
    out_ref[...] = jnp.where(mine, own_ref[:1], back_ref[:1])


def hidden_kernel(pairs, chunk, column_ref, up_hbm, hidden_hbm, w_hbm, *refs):
    got_refs = refs[: len(pairs)]
    out_ref, own_score, got_score = refs[len(pairs) : len(pairs) + 3]
    routed_ref, hidden_ref, w_ref, sems = refs[len(pairs) + 3 :]
    tokens = up_hbm.shape[0]
    hidden_units = w_ref.shape[0]
    width = 2 * LANES
    blocks = hidden_units // width
    expert = lax.axis_index("expert")
    top = pltpu.make_async_copy(up_hbm, routed_ref.at[pl.ds(0, tokens)], sems.at[blocks])
    stored = pltpu.make_async_copy(hidden_hbm, hidden_ref, sems.at[blocks + 1])
    loads = []
    for i in range(blocks):
        rows = pl.ds(i * width, width)
        loads.append(pltpu.make_async_copy(w_hbm.at[rows], w_ref.at[rows], sems.at[i]))
    top.start()
    loads[0].start()
    stored.start()
    for load in loads[1:]:
        load.start()
    for got_ref, pair in zip(got_refs, pairs):
        for i, k in enumerate(pair):
            routed_ref[tokens:, pl.ds(chunk_start(k, chunk), chunk)] = got_ref[:, i * chunk : (i + 1) * chunk]
    column = len(pairs[0]) * chunk
    weights = [column_ref[:, :1], got_refs[0][:, column : column + 1].astype(jnp.float32)]
    scores = [None, None]
    top.wait()
    for i in range(blocks):
        loads[i].wait()
        backward = lax.dot_general(
            routed_ref[...], w_ref[i * width : (i + 1) * width, :], TURNED, preferred_element_type=jnp.float32
        )
        if i == 0:
            stored.wait()
        gate_cols = slice(i * width, (i + 1) * width)
        up_cols = slice(hidden_units + i * width, hidden_units + (i + 1) * width)
        for part in range(2):
            back = backward[part * tokens : (part + 1) * tokens]
            rows = pl.ds(pl.multiple_of((expert ^ part) * tokens, tokens), tokens)
            gate = hidden_ref[rows, gate_cols].astype(jnp.float32)
            up = hidden_ref[rows, up_cols].astype(jnp.float32)
            sig = jax.nn.sigmoid(gate)
            act = (gate * sig * up).astype(jnp.bfloat16).astype(jnp.float32)
            score = jnp.sum(back * act, axis=1, keepdims=True)
            scores[part] = score if i == 0 else scores[part] + score
            grad = weights[part] * back
            out_ref[rows, gate_cols] = (grad * up * sig * (1.0 + gate * (1.0 - sig))).astype(jnp.bfloat16)
            out_ref[rows, up_cols] = (grad * gate * sig).astype(jnp.bfloat16)
    for score, ref in zip(scores, (own_score, got_score)):
        ref[...] = jnp.broadcast_to(score, (tokens, LANES)).T[:8]


def both_experts(upstream, combine_weights, expert_ids, saved_hidden, down_weight):
    tokens, features = upstream.shape
    n = lax.axis_size("dp")
    outer = n // INNER
    chunk, piece = features // outer, features // n
    hidden_units = down_weight.shape[1]
    stored, weights = saved_hidden[0], down_weight[0]
    ids, combine = expert_ids.T, combine_weights.T
    flip = [(0, 1), (1, 0)]
    cross = lambda value: lax.ppermute(value, "expert", flip)
    swap = lambda value, bit: lax.ppermute(value, "dp", [(i, i ^ bit) for i in range(n)])
    rows = stored.shape[0]
    bf16, f32 = jnp.bfloat16, jnp.float32
    pairs = ((3,), (2,), (1,), (0,))
    sides = (hidden_units,)

    order = tuple(pair[0] for pair in pairs)
    first, *mine = call((
        functools.partial(first_kernel, order[0], chunk),
        [upstream, stored, ids, combine],
        [((tokens, chunk + LANES), bf16)] + [((rows, hidden_units // 2), bf16)] * 2,
        [pltpu.VMEM((rows, 2 * hidden_units), bf16), pltpu.SemaphoreType.DMA((3,))],
        [HBM, HBM, LOAD, LOAD],
    ))
    column, *own = call((
        functools.partial(own_kernel, order, chunk),
        [upstream, ids, combine],
        [((tokens, LANES), f32)] + [((chunk, tokens), bf16)] * outer + [((tokens, chunk), bf16)] * (outer - 1),
        [pltpu.VMEM((outer, tokens, chunk), bf16), pltpu.SemaphoreType.DMA((outer,))],
        [HBM, LOAD, LOAD],
    ), waits=(first,))
    send, own = [first] + own[outer:], own[:outer]

    def split_job(i):
        return (
            functools.partial(split_kernel, chunk),
            [got[i], got[0], own[i]],
            [((piece, 2 * tokens), bf16)] * INNER,
            [pltpu.VMEM((chunk, tokens), bf16)],
            None,
        )

    def spread(cut):
        return [cut[0]] + [swap(cut[j], j) for j in range(1, INNER)], cut[0]

    def split(i, *waits):
        return spread(call(split_job(i), waits=waits))

    def parts(i, kind, cuts, *adds):
        kernel = functools.partial(parts_kernel, len(adds))
        args = [*pays[i], *acts[0], *acts[1], *adds]
        return kernel, args, [((piece, width), kind) for width in cuts], [], None

    got, pays, marks = {}, {}, {}
    got[0] = cross(send[0])
    acts = [[mine[h], swap(mine[h], 1), swap(mine[h], 2)] for h in range(2)]
    pays[0], marks[0] = split(0)
    got[1] = cross(after(send[1], marks[0]))
    acts[0].append(swap(after(acts[0][2], marks[0]), 1))
    acts[1].append(swap(after(acts[1][2], acts[0][3]), 1))
    far, *cut = call(parts(0, bf16, (hidden_units,)), split_job(1))
    near = swap(far, INNER)
    pays[1], marks[1] = spread(cut)
    got[2] = cross(after(send[2], acts[0][3]))
    pays[2], marks[2] = split(2, far)
    wide, = call(parts(1, bf16, (hidden_units,), near))
    last = [swap(wide, 2 * INNER)]
    got[3] = cross(after(send[3], marks[2]))
    *side, _0, _1, _2, _3 = call(parts(2, bf16, sides), split_job(3), waits=(wide,))
    pays[3], marks[3] = spread((_0, _1, _2, _3))
    side = [swap(part, INNER) for part in side]

    grad_hidden, own_score, got_score = call(
        (
            functools.partial(hidden_kernel, pairs, chunk),
            [column, upstream, stored, weights, *[got[i] for i in range(outer)]],
            [(stored.shape, bf16), ((8, tokens), f32), ((8, tokens), f32)],
            [
                pltpu.VMEM((rows, features), bf16),
                pltpu.VMEM(stored.shape, bf16),
                pltpu.VMEM(weights.shape, bf16),
                pltpu.SemaphoreType.DMA((hidden_units // (2 * LANES) + 2,)),
            ],
            [VMEM, HBM, HBM, HBM] + [VMEM] * outer,
        ),
        waits=(marks[3],), vmem=18,
    )
    back_score = cross(got_score)
    base, = call(parts(3, f32, (hidden_units,)), waits=(own_score,))
    grad_probs, = call((probs_kernel, [ids, own_score, back_score], [(ids.shape, f32)], [], None), waits=last)
    grad_down, = call((
        functools.partial(final_kernel, len(side)), [base, *side, *last],
        [((piece, hidden_units), f32)], [], None,
    ))
    return grad_down[None], grad_hidden[None], grad_probs.T


def any_experts(upstream, combine_weights, expert_ids, saved_hidden, down_weight):
    tok_rows, features = upstream.shape
    experts = lax.axis_size("expert")
    hidden_units = down_weight.shape[1]
    capacity = saved_hidden.shape[1] // experts
    labels = lax.broadcasted_iota(jnp.int32, (1, 1, experts), 2)
    matched = expert_ids[:, :, None] == labels
    member = jnp.sum(matched.astype(jnp.int32), axis=1)
    slot_rank = jnp.cumsum(member, axis=0) - member
    token_iota = lax.broadcasted_iota(jnp.int32, (tok_rows, experts, capacity), 0)
    slot_iota = lax.broadcasted_iota(jnp.int32, (tok_rows, experts, capacity), 2)
    placed = (member[:, :, None] == 1) & (slot_rank[:, :, None] == slot_iota)
    source = jnp.sum(jnp.where(placed, token_iota, 0), axis=0)
    filled = jnp.any(placed, axis=0)
    token_weight = jnp.sum(
        jnp.where(matched, combine_weights[:, :, None].astype(jnp.float32), 0.0), axis=1
    )
    send_rows = jnp.where(filled[:, :, None], upstream[source], jnp.zeros((), jnp.bfloat16))
    send_weight = jnp.where(
        filled, jnp.take_along_axis(token_weight.T, source, axis=1), 0.0
    ).astype(jnp.bfloat16)
    got_rows, got_weight = (
        lax.all_to_all(send_rows, "expert", split_axis=0, concat_axis=0, tiled=True),
        lax.all_to_all(send_weight, "expert", split_axis=0, concat_axis=0, tiled=True),
    )
    routed = got_rows.reshape(experts * capacity, features)
    row_weight = got_weight.reshape(experts * capacity, 1).astype(jnp.float32)
    stored = saved_hidden[0]
    gate_pre = stored[:, :hidden_units].astype(jnp.float32)
    up_pre = stored[:, hidden_units:].astype(jnp.float32)
    sigmoid_gate = jax.nn.sigmoid(gate_pre)
    activated = (gate_pre * sigmoid_gate * up_pre).astype(jnp.bfloat16)
    scaled = (row_weight * routed.astype(jnp.float32)).astype(jnp.bfloat16)
    weights = down_weight[0]
    backward = lax.dot_general(
        routed, weights, (((1,), (1,)), ((), ())), preferred_element_type=jnp.float32
    )
    grad_act = row_weight * backward
    grad_gate = grad_act * up_pre * sigmoid_gate * (1.0 + gate_pre * (1.0 - sigmoid_gate))
    grad_up = grad_act * gate_pre * sigmoid_gate
    grad_hidden = jnp.concatenate([grad_gate, grad_up], axis=1).astype(jnp.bfloat16)
    outputs = jnp.dot(activated, weights, preferred_element_type=jnp.float32)
    scores = jnp.sum(routed.astype(jnp.float32) * outputs, axis=1)
    returned = lax.all_to_all(
        scores.reshape(experts, capacity), "expert", split_axis=0, concat_axis=0, tiled=True
    )
    slot_of = jnp.sum(jnp.where(matched, slot_rank[:, None, :], 0), axis=2)
    flat_index = expert_ids * capacity + slot_of
    score_table = returned.reshape(experts * capacity)
    cell_ids = lax.broadcasted_iota(jnp.int32, (1, 1, experts * capacity), 2)
    grad_probs = jnp.sum(
        jnp.where(flat_index[:, :, None] == cell_ids, score_table[None, None, :], 0.0), axis=2
    )
    grad_down = lax.psum_scatter(
        contract_rows(scaled, activated), "dp", scatter_dimension=0, tiled=True
    )
    return (grad_down[None], grad_hidden[None], grad_probs)


def local(upstream, combine_weights, expert_ids, saved_hidden, down_weight):
    tokens, features = upstream.shape
    n = lax.axis_size("dp")
    outer = n // INNER
    every_token_to_both = (
        lax.axis_size("expert") == 2
        and expert_ids.shape[1] == 2
        and saved_hidden.shape[1] == 2 * tokens
        and tokens == LANES
    )
    splits = n == 4 * INNER and features % (n * 16) == 0 and features % (outer * LANES) == 0
    hidden_units = down_weight.shape[1]
    if every_token_to_both and splits and hidden_units % (4 * LANES) == 0:
        return both_experts(upstream, combine_weights, expert_ids, saved_hidden, down_weight)
    return any_experts(upstream, combine_weights, expert_ids, saved_hidden, down_weight)


def solution(mesh):
    return jax.shard_map(
        local,
        mesh=mesh,
        in_specs=(
            P(("expert", "dp"), None),
            P(("expert", "dp"), None),
            P(("expert", "dp"), None),
            P("expert", "dp", None),
            P("expert", None, None),
        ),
        out_specs=(P("expert", "dp", None), P("expert", "dp", None), P(("expert", "dp"), None)),
        check_vma=False,
    )
```

```python
import functools

import jax
import jax.numpy as jnp
from jax import lax
from jax.experimental import pallas as pl
from jax.experimental.pallas import tpu as pltpu
from jax.sharding import PartitionSpec as P

INNER = 4
LANES = 128
VMEM = pl.BlockSpec(memory_space=pltpu.VMEM)
HBM = pl.BlockSpec(memory_space=pltpu.HBM)
LOAD = pl.BlockSpec(memory_space=pltpu.VMEM)
ANY = pl.BlockSpec(memory_space=pl.ANY)
TURNED = (((1,), (1,)), ((), ()))


def contract_rows(left_rows, right_rows):
    return lax.dot_general(
        left_rows, right_rows, (((0,), (0,)), ((), ())), preferred_element_type=jnp.float32
    )


def after(value, *others):
    return lax.optimization_barrier((value, *others))[0]


def call(*jobs, waits=(), vmem=8):
    specs = [spec for job in jobs for spec in job[4] or [VMEM] * len(job[1])]
    args = [arg for job in jobs for arg in job[1]]
    outs = tuple(jax.ShapeDtypeStruct(*out) for job in jobs for out in job[2])
    scratch = [item for job in jobs for item in job[3]]

    def body(*refs):
        ins, rest = refs[: len(args)], refs[len(args) + len(waits) :]
        out_refs, temps = rest[: len(outs)], rest[len(outs) :]
        for kernel, job_args, job_outs, job_scratch, _ in jobs:
            x, y, z = len(job_args), len(job_outs), len(job_scratch)
            kernel(*ins[:x], *out_refs[:y], *temps[:z])
            ins, out_refs, temps = ins[x:], out_refs[y:], temps[z:]

    place = lambda arg, spec: arg if spec is VMEM else pltpu.with_memory_space_constraint(arg, pltpu.HBM)
    return pl.pallas_call(
        body,
        out_shape=outs,
        in_specs=specs + [ANY] * len(waits),
        out_specs=tuple(VMEM for _ in outs),
        scratch_shapes=scratch,
        compiler_params=pltpu.CompilerParams(vmem_limit_bytes=vmem << 20),
    )(*[place(*pair) for pair in zip(args, specs)], *waits)


def chunk_start(k, chunk):
    group = lax.axis_index("dp") // INNER
    return pl.multiple_of((group ^ k) * chunk, LANES)


def token_weight(ids_ref, weights_ref, expert):
    picked = jnp.where(ids_ref[...] == expert, weights_ref[...].astype(jnp.float32), 0.0)
    lanes = jnp.sum(picked, axis=0, keepdims=True)
    return jnp.broadcast_to(lanes, (LANES, lanes.shape[1])).T


def first_kernel(k, chunk, up_hbm, hidden_hbm, ids_ref, weights_ref, send_ref, act0_ref, act1_ref, hidden_ref, sems):
    cols = pl.ds(chunk_start(k, chunk), chunk)
    rows = pltpu.make_async_copy(up_hbm.at[:, cols], send_ref.at[:, pl.ds(0, chunk)], sems.at[0])
    half, hidden_units = hidden_ref.shape[0] // 2, hidden_ref.shape[1] // 2
    loads = []
    for part in range(2):
        span = pl.ds(part * half, half)
        loads.append(pltpu.make_async_copy(hidden_hbm.at[span], hidden_ref.at[span], sems.at[1 + part]))
    for load in loads:
        load.start()
    rows.start()
    expert = lax.axis_index("expert")
    send_ref[:, chunk:] = token_weight(ids_ref, weights_ref, 1 - expert).astype(jnp.bfloat16)
    for part in range(2):
        loads[part].wait()
        target = pl.ds(pl.multiple_of((expert ^ part) * half, half), half)
        gate = hidden_ref[part * half : (part + 1) * half, :hidden_units].astype(jnp.float32)
        up = hidden_ref[part * half : (part + 1) * half, hidden_units:].astype(jnp.float32)
        act = (gate * jax.nn.sigmoid(gate) * up).astype(jnp.bfloat16)
        for i, act_ref in enumerate((act0_ref, act1_ref)):
            width = act_ref.shape[1]
            act_ref[target, :] = act[:, i * width : (i + 1) * width]
    rows.wait()


def own_kernel(order, chunk, up_hbm, ids_ref, weights_ref, *refs):
    column_ref, kept_ref, refs = refs[0], refs[1], refs[2:]
    kept_ref[...] = ids_ref[...]
    own_refs, send_refs = refs[: len(order)], refs[len(order) : -2]
    up_ref, sems = refs[-2:]
    loads = []
    for i, k in enumerate(order):
        cols = pl.ds(chunk_start(k, chunk), chunk)
        loads.append(pltpu.make_async_copy(up_hbm.at[:, cols], up_ref.at[i], sems.at[i]))
        loads[i].start()
    weight = token_weight(ids_ref, weights_ref, lax.axis_index("expert"))
    column_ref[...] = weight
    weight = weight[:, :1]
    for i in range(len(order)):
        loads[i].wait()
        rows = up_ref[i]
        if i:
            send_refs[i - 1][...] = rows
        own_refs[i][...] = (weight * rows.astype(jnp.float32)).astype(jnp.bfloat16).T


def split_kernel(chunk, got_ref, first_ref, *refs):
    owns, pays, scaled_ref = refs[: -INNER - 1], refs[-INNER - 1 : -1], refs[-1]
    column = first_ref.shape[1] - LANES
    weight = first_ref[:, column : column + 1].astype(jnp.float32)
    piece = chunk // INNER
    mine = lax.axis_index("dp") % INNER
    for i, own_ref in enumerate(owns):
        scaled = weight * got_ref[:, i * chunk : (i + 1) * chunk].astype(jnp.float32)
        scaled_ref[...] = scaled.astype(jnp.bfloat16).T
        for j in range(INNER):
            rows = pl.ds(pl.multiple_of((mine ^ j) * piece, 16), piece)
            pays[j][i * piece : (i + 1) * piece, :LANES] = own_ref[rows, :]
            pays[j][i * piece : (i + 1) * piece, LANES:] = scaled_ref[rows, :]


def parts_kernel(adds, *refs):
    pays, acts, rest = refs[:INNER], refs[INNER : 3 * INNER], refs[3 * INNER :]
    adds, outs = rest[:adds], rest[adds:]
    total = []
    for half in (acts[:INNER], acts[INNER:]):
        terms = [jnp.dot(p[...], a[...], preferred_element_type=jnp.float32) for p, a in zip(pays, half)]
        total.append(functools.reduce(jnp.add, terms))
    total = jnp.concatenate(total, axis=1)
    for add in adds:
        total = total + add[...].astype(jnp.float32)
    start = 0
    for out_ref in outs:
        stop = start + out_ref.shape[1]
        out_ref[...] = total[:, start:stop].astype(out_ref.dtype)
        start = stop


def final_kernel(sides, base_ref, *refs):
    terms, out_ref = refs[:-1], refs[-1]
    side, last = [
        jnp.concatenate([ref[...].astype(jnp.float32) for ref in part], axis=1)
        for part in (terms[:sides], terms[sides:])
    ]
    out_ref[...] = base_ref[...] + (side + last)


def probs_kernel(ids_ref, own_ref, back_ref, out_ref):
    mine = ids_ref[...] == lax.axis_index("expert")
    out_ref[...] = jnp.where(mine, own_ref[:1], back_ref[:1])


def hidden_kernel(pairs, chunk, column_ref, up_hbm, hidden_hbm, w_hbm, *refs):
    got_refs = refs[: len(pairs)]
    out_ref, own_score, got_score = refs[len(pairs) : len(pairs) + 3]
    routed_ref, hidden_ref, w_ref, sems = refs[len(pairs) + 3 :]
    tokens = up_hbm.shape[0]
    hidden_units = w_ref.shape[0]
    width = 2 * LANES
    blocks = hidden_units // width
    expert = lax.axis_index("expert")
    top = pltpu.make_async_copy(up_hbm, routed_ref.at[pl.ds(0, tokens)], sems.at[blocks])
    stored = pltpu.make_async_copy(hidden_hbm, hidden_ref, sems.at[blocks + 1])
    loads = []
    for i in range(blocks):
        rows = pl.ds(i * width, width)
        loads.append(pltpu.make_async_copy(w_hbm.at[rows], w_ref.at[rows], sems.at[i]))
    top.start()
    loads[0].start()
    stored.start()
    for load in loads[1:]:
        load.start()
    for got_ref, pair in zip(got_refs, pairs):
        for i, k in enumerate(pair):
            routed_ref[tokens:, pl.ds(chunk_start(k, chunk), chunk)] = got_ref[:, i * chunk : (i + 1) * chunk]
    column = len(pairs[0]) * chunk
    weights = [column_ref[:, :1], got_refs[0][:, column : column + 1].astype(jnp.float32)]
    scores = [None, None]
    top.wait()
    for i in range(blocks):
        loads[i].wait()
        backward = lax.dot_general(
            routed_ref[...], w_ref[i * width : (i + 1) * width, :], TURNED, preferred_element_type=jnp.float32
        )
        if i == 0:
            stored.wait()
        gate_cols = slice(i * width, (i + 1) * width)
        up_cols = slice(hidden_units + i * width, hidden_units + (i + 1) * width)
        for part in range(2):
            back = backward[part * tokens : (part + 1) * tokens]
            rows = pl.ds(pl.multiple_of((expert ^ part) * tokens, tokens), tokens)
            gate = hidden_ref[rows, gate_cols].astype(jnp.float32)
            up = hidden_ref[rows, up_cols].astype(jnp.float32)
            sig = jax.nn.sigmoid(gate)
            act = (gate * sig * up).astype(jnp.bfloat16).astype(jnp.float32)
            score = jnp.sum(back * act, axis=1, keepdims=True)
            scores[part] = score if i == 0 else scores[part] + score
            grad = weights[part] * back
            out_ref[rows, gate_cols] = (grad * up * sig * (1.0 + gate * (1.0 - sig))).astype(jnp.bfloat16)
            out_ref[rows, up_cols] = (grad * gate * sig).astype(jnp.bfloat16)
    for score, ref in zip(scores, (own_score, got_score)):
        ref[...] = jnp.broadcast_to(score, (tokens, LANES)).T[:8]


def both_experts(upstream, combine_weights, expert_ids, saved_hidden, down_weight):
    tokens, features = upstream.shape
    n = lax.axis_size("dp")
    outer = n // INNER
    chunk, piece = features // outer, features // n
    hidden_units = down_weight.shape[1]
    stored, weights = saved_hidden[0], down_weight[0]
    ids, combine = expert_ids.T, combine_weights.T
    flip = [(0, 1), (1, 0)]
    cross = lambda value: lax.ppermute(value, "expert", flip)
    swap = lambda value, bit: lax.ppermute(value, "dp", [(i, i ^ bit) for i in range(n)])
    rows = stored.shape[0]
    bf16, f32 = jnp.bfloat16, jnp.float32
    pairs = ((3,), (2,), (1,), (0,))
    sides = (hidden_units,)

    order = tuple(pair[0] for pair in pairs)
    first, *mine = call((
        functools.partial(first_kernel, order[0], chunk),
        [upstream, stored, ids, combine],
        [((tokens, chunk + LANES), bf16)] + [((rows, hidden_units // 2), bf16)] * 2,
        [pltpu.VMEM((rows, 2 * hidden_units), bf16), pltpu.SemaphoreType.DMA((3,))],
        [HBM, HBM, LOAD, LOAD],
    ))
    column, kept, *own = call((
        functools.partial(own_kernel, order, chunk),
        [upstream, ids, combine],
        [((tokens, LANES), f32), (ids.shape, jnp.int32)] + [((chunk, tokens), bf16)] * outer + [((tokens, chunk), bf16)] * (outer - 1),
        [pltpu.VMEM((outer, tokens, chunk), bf16), pltpu.SemaphoreType.DMA((outer,))],
        [HBM, LOAD, LOAD],
    ), waits=(first,))
    send, own = [first] + own[outer:], own[:outer]

    def split_job(i):
        return (
            functools.partial(split_kernel, chunk),
            [got[i], got[0], own[i]],
            [((piece, 2 * tokens), bf16)] * INNER,
            [pltpu.VMEM((chunk, tokens), bf16)],
            None,
        )

    def spread(cut):
        return [cut[0]] + [swap(cut[j], j) for j in range(1, INNER)], cut[0]

    def split(i, *waits):
        return spread(call(split_job(i), waits=waits))

    def parts(i, kind, cuts, *adds):
        kernel = functools.partial(parts_kernel, len(adds))
        args = [*pays[i], *acts[0], *acts[1], *adds]
        return kernel, args, [((piece, width), kind) for width in cuts], [], None

    got, pays, marks = {}, {}, {}
    got[0] = cross(send[0])
    acts = [[mine[h], swap(mine[h], 1), swap(mine[h], 2)] for h in range(2)]
    pays[0], marks[0] = split(0)
    got[1] = cross(after(send[1], marks[0]))
    acts[0].append(swap(after(acts[0][2], marks[0]), 1))
    acts[1].append(swap(after(acts[1][2], acts[0][3]), 1))
    far, *cut = call(parts(0, bf16, (hidden_units,)), split_job(1))
    near = swap(far, INNER)
    pays[1], marks[1] = spread(cut)
    got[2] = cross(after(send[2], acts[0][3]))
    pays[2], marks[2] = split(2, far)
    wide, = call(parts(1, bf16, (hidden_units,), near))
    last = [swap(wide, 2 * INNER)]
    got[3] = cross(after(send[3], marks[2]))
    *side, _0, _1, _2, _3 = call(parts(2, bf16, sides), split_job(3), waits=(wide,))
    pays[3], marks[3] = spread((_0, _1, _2, _3))
    side = [swap(part, INNER) for part in side]

    grad_hidden, own_score, got_score = call(
        (
            functools.partial(hidden_kernel, pairs, chunk),
            [column, upstream, stored, weights, *[got[i] for i in range(outer)]],
            [(stored.shape, bf16), ((8, tokens), f32), ((8, tokens), f32)],
            [
                pltpu.VMEM((rows, features), bf16),
                pltpu.VMEM(stored.shape, bf16),
                pltpu.VMEM(weights.shape, bf16),
                pltpu.SemaphoreType.DMA((hidden_units // (2 * LANES) + 2,)),
            ],
            [VMEM, HBM, HBM, HBM] + [VMEM] * outer,
        ),
        waits=(marks[3],), vmem=18,
    )
    back_score = cross(got_score)
    base, = call(parts(3, f32, (hidden_units,)), waits=(own_score,))
    grad_probs, = call((probs_kernel, [kept, own_score, back_score], [(ids.shape, f32)], [], None), waits=last)
    grad_down, = call((
        functools.partial(final_kernel, len(side)), [base, *side, *last],
        [((piece, hidden_units), f32)], [], None,
    ))
    return grad_down[None], grad_hidden[None], grad_probs.T


def any_experts(upstream, combine_weights, expert_ids, saved_hidden, down_weight):
    tok_rows, features = upstream.shape
    experts = lax.axis_size("expert")
    hidden_units = down_weight.shape[1]
    capacity = saved_hidden.shape[1] // experts
    labels = lax.broadcasted_iota(jnp.int32, (1, 1, experts), 2)
    matched = expert_ids[:, :, None] == labels
    member = jnp.sum(matched.astype(jnp.int32), axis=1)
    slot_rank = jnp.cumsum(member, axis=0) - member
    token_iota = lax.broadcasted_iota(jnp.int32, (tok_rows, experts, capacity), 0)
    slot_iota = lax.broadcasted_iota(jnp.int32, (tok_rows, experts, capacity), 2)
    placed = (member[:, :, None] == 1) & (slot_rank[:, :, None] == slot_iota)
    source = jnp.sum(jnp.where(placed, token_iota, 0), axis=0)
    filled = jnp.any(placed, axis=0)
    token_weight = jnp.sum(
        jnp.where(matched, combine_weights[:, :, None].astype(jnp.float32), 0.0), axis=1
    )
    send_rows = jnp.where(filled[:, :, None], upstream[source], jnp.zeros((), jnp.bfloat16))
    send_weight = jnp.where(
        filled, jnp.take_along_axis(token_weight.T, source, axis=1), 0.0
    ).astype(jnp.bfloat16)
    got_rows, got_weight = (
        lax.all_to_all(send_rows, "expert", split_axis=0, concat_axis=0, tiled=True),
        lax.all_to_all(send_weight, "expert", split_axis=0, concat_axis=0, tiled=True),
    )
    routed = got_rows.reshape(experts * capacity, features)
    row_weight = got_weight.reshape(experts * capacity, 1).astype(jnp.float32)
    stored = saved_hidden[0]
    gate_pre = stored[:, :hidden_units].astype(jnp.float32)
    up_pre = stored[:, hidden_units:].astype(jnp.float32)
    sigmoid_gate = jax.nn.sigmoid(gate_pre)
    activated = (gate_pre * sigmoid_gate * up_pre).astype(jnp.bfloat16)
    scaled = (row_weight * routed.astype(jnp.float32)).astype(jnp.bfloat16)
    weights = down_weight[0]
    backward = lax.dot_general(
        routed, weights, (((1,), (1,)), ((), ())), preferred_element_type=jnp.float32
    )
    grad_act = row_weight * backward
    grad_gate = grad_act * up_pre * sigmoid_gate * (1.0 + gate_pre * (1.0 - sigmoid_gate))
    grad_up = grad_act * gate_pre * sigmoid_gate
    grad_hidden = jnp.concatenate([grad_gate, grad_up], axis=1).astype(jnp.bfloat16)
    outputs = jnp.dot(activated, weights, preferred_element_type=jnp.float32)
    scores = jnp.sum(routed.astype(jnp.float32) * outputs, axis=1)
    returned = lax.all_to_all(
        scores.reshape(experts, capacity), "expert", split_axis=0, concat_axis=0, tiled=True
    )
    slot_of = jnp.sum(jnp.where(matched, slot_rank[:, None, :], 0), axis=2)
    flat_index = expert_ids * capacity + slot_of
    score_table = returned.reshape(experts * capacity)
    cell_ids = lax.broadcasted_iota(jnp.int32, (1, 1, experts * capacity), 2)
    grad_probs = jnp.sum(
        jnp.where(flat_index[:, :, None] == cell_ids, score_table[None, None, :], 0.0), axis=2
    )
    grad_down = lax.psum_scatter(
        contract_rows(scaled, activated), "dp", scatter_dimension=0, tiled=True
    )
    return (grad_down[None], grad_hidden[None], grad_probs)


def local(upstream, combine_weights, expert_ids, saved_hidden, down_weight):
    tokens, features = upstream.shape
    n = lax.axis_size("dp")
    outer = n // INNER
    every_token_to_both = (
        lax.axis_size("expert") == 2
        and expert_ids.shape[1] == 2
        and saved_hidden.shape[1] == 2 * tokens
        and tokens == LANES
    )
    splits = n == 4 * INNER and features % (n * 16) == 0 and features % (outer * LANES) == 0
    hidden_units = down_weight.shape[1]
    if every_token_to_both and splits and hidden_units % (4 * LANES) == 0:
        return both_experts(upstream, combine_weights, expert_ids, saved_hidden, down_weight)
    return any_experts(upstream, combine_weights, expert_ids, saved_hidden, down_weight)


def solution(mesh):
    return jax.shard_map(
        local,
        mesh=mesh,
        in_specs=(
            P(("expert", "dp"), None),
            P(("expert", "dp"), None),
            P(("expert", "dp"), None),
            P("expert", "dp", None),
            P("expert", None, None),
        ),
        out_specs=(P("expert", "dp", None), P("expert", "dp", None), P(("expert", "dp"), None)),
        check_vma=False,
    )
```
